32 devices in a mesh: gx: 4 (over z), gy: 2 (over x), gz: 4 (over y, core).
Axes of the slice: x: 2, y: 2, z: 4, core: 2. Of those that a mesh axis runs over, the one named last changes fastest.
Arguments:
- bases: float32 [4, 2, 4, 1024, 128], P('gx', 'gy', 'gz'), may hold values from -1 to 1, as said below
- ranks: int32 [4, 2, 4], P('gx', 'gy', 'gz'), may hold values from 64 to 128
- couplings: bfloat16 [4, 2, 4, 5, 1024, 1024], P('gx', 'gy', 'gz'), may hold values from -6 to 6
- vectors: float32 [4, 2, 4, 1024, 256], P('gx', 'gy', 'gz'), may hold values from -0.1875 to 0.1875
Outputs:
- projected: float32 [4, 2, 4, 5, 128, 128], P('gx', 'gy', 'gz')
- applied: float32 [4, 2, 4, 1024, 256], P('gx', 'gy', 'gz')
The draws below stay inside these ranges and needn't reach their ends.
Inputs may be any that keep to these rules, and one draw needn't show every extreme that they name: `bases`: for each subdomain the 1024 x 128 matrix has orthonormal columns.
All inputs are finite; a program needn't handle non-finite values.
Results may differ from the reference program's by a relative error of at most 0.0003.
Values sent between devices are 32-bit elements; how exact they have to be, the bound alone decides.
A program may use at most 64 MiB of HBM per device.

```python
import jax
import jax.numpy as jnp
from jax import lax

M = 1024
K = 128
R = 256
NB = 5
N_GX = 4
N_GY = 2
N_GZ = 4


def orthonormal_columns(sample):
    return jnp.linalg.qr(sample)[0]


def draw_bases(key, part):
    device_total = N_GX * N_GY * N_GZ
    sample = jax.random.normal(key, (device_total, M, K), jnp.float32)
    orthonormal = jax.vmap(orthonormal_columns)(sample)
    return orthonormal.reshape(N_GX, N_GY, N_GZ, M, K).astype(jnp.float32)


def touch_ends(array, stream_key, least, top_value):
    longest = array.shape.index(max(array.shape))
    spots = []
    for shift in (0, 1):
        where = [jax.random.randint(jax.random.fold_in(stream_key, axis), (), 0, length) for axis, length in enumerate(array.shape)]
        where[longest] = (where[longest] + shift) % array.shape[longest]
        spots.append(tuple(where))
    return array.at[spots[0]].set(least).at[spots[1]].set(top_value)


def steps_of(rng, shape, split, low, top_value):
    def one(dim, parts):
        heights = jax.random.uniform(jax.random.fold_in(jax.random.fold_in(rng, 6), dim), (parts,), jnp.float32, low / len(split), top_value / len(split))
        return jnp.repeat(jnp.exp(heights), shape[dim] // parts).reshape((-1,) + (1,) * (len(shape) - dim - 1))

    gain = one(*split[0])
    for cut in split[1:]:
        gain = gain * one(*cut)
    return gain


def normal_values(own_key, extent, deviation, bound, pieces=(), kind=jnp.bfloat16):
    drawn = deviation * jax.random.normal(own_key, extent, jnp.float32)
    if pieces:
        drawn = drawn * steps_of(own_key, extent, pieces, -0.22, 0.18)
    return jnp.clip(drawn, -bound, bound).astype(kind)


def setup_inputs(seed: int = 0) -> dict:
    seeds = jax.random.split(jax.random.key(seed), 5)
    return {
        "bases": draw_bases(jax.random.fold_in(seeds[4], 71), 0),
        "ranks": touch_ends(jax.random.randint(seeds[1], (N_GX, N_GY, N_GZ), K // 2, K + 1), jax.random.fold_in(seeds[1], 1), K // 2, K).astype(jnp.int32),
        "couplings": normal_values(seeds[2], (N_GX, N_GY, N_GZ, NB, M, M), 1.0, 6.0, ((0, 4), (1, 2), (2, 4))),
        "vectors": normal_values(seeds[3], (N_GX, N_GY, N_GZ, M, R), M ** -0.5, 0.1875, ((0, 4), (1, 2), (2, 4)), jnp.float32),
    }


OFFSET_LIST = ((1, 0, 0), (0, 1, 0), (0, 0, 1), (1, 1, 0), (1, 0, 1), (0, 1, 1), (1, 1, 1))

def reference(bases, ranks, couplings, vectors):
    columns = jnp.arange(K, dtype=jnp.int32)
    keep = (columns < ranks[..., None]).astype(jnp.float32)
    masked = bases * keep[..., None, :]
    joined = jnp.concatenate([masked, vectors], axis=-1)
    padded = jnp.pad(joined, ((0, 1), (0, 1), (0, 1), (0, 0), (0, 0)))
    device_total = N_GX * N_GY * N_GZ
    neighbour_list = []
    for slot in range(NB):
        shift_x, shift_y, shift_z = OFFSET_LIST[slot]
        moved = padded[shift_x:shift_x + N_GX, shift_y:shift_y + N_GY, shift_z:shift_z + N_GZ]
        neighbour_list.append(moved.reshape(device_total, M, K + R))
    neighbours = jnp.stack(neighbour_list, axis=1)
    flat_bases = masked.reshape(device_total, M, K)
    flat_couplings = couplings.reshape(device_total, NB, M, M)

    def one_device(index):
        own_basis = flat_bases[index]

        def one_block(slot):
            neighbour = neighbours[index, slot]
            coupling = flat_couplings[index, slot].astype(jnp.float32)
            coupled = jnp.dot(coupling, neighbour[:, :K], precision=lax.Precision.HIGHEST)
            acted = jnp.dot(coupling, neighbour[:, K:], precision=lax.Precision.HIGHEST)
            return (jnp.dot(own_basis.T, coupled, precision=lax.Precision.HIGHEST), acted)
        blocks, acted = lax.map(one_block, jnp.arange(NB, dtype=jnp.int32))
        return (blocks, jnp.sum(acted, axis=0))
    result, applied = lax.map(one_device, jnp.arange(device_total, dtype=jnp.int32))
    return (result.reshape(N_GX, N_GY, N_GZ, NB, K, K), applied.reshape(N_GX, N_GY, N_GZ, M, R))
```

```python
import functools

import jax
import jax.numpy as jnp
from jax import lax
from jax.experimental import pallas as pl
from jax.experimental.pallas import tpu as pltpu
from jax.sharding import PartitionSpec as P

OFFSET_LIST = ((1, 0, 0), (0, 1, 0), (0, 0, 1), (1, 1, 0), (1, 0, 1), (0, 1, 1), (1, 1, 1))
AXES = ("gx", "gy", "gz")
X, Y, Z, XY, XZ = range(5)
LEFT_ORDER = (XY, Y, X, XZ, Z)


def split2(value):
    high = value.astype(jnp.bfloat16)
    low = (value - high.astype(jnp.float32)).astype(jnp.bfloat16)
    return high, low


def dot32(left, right):
    return jnp.dot(left, right, preferred_element_type=jnp.float32)


def kernel(
    sizes, ranks_ref, bases_ref, couplings_ref, vectors_ref, projected_ref, applied_ref,
    basis, stacked, basis_parts, blocks, values, left_out, left_in, back_out, back_in, total,
    basis_sem, block_sem, value_send, value_recv, left_send, left_recv, back_send, back_recv,
):
    count, m, k = blocks.shape[0], basis.shape[0], basis.shape[1]
    r = total.shape[1]
    half = m // 2
    place = [lax.axis_index(name) for name in AXES]
    has_up = [p < n - 1 for p, n in zip(place, sizes)]
    has_down = [p > 0 for p in place]

    def every(flags, offset):
        out = None
        for flag, o in zip(flags, offset):
            if o:
                out = flag if out is None else jnp.logical_and(out, flag)
        return out

    up = [every(has_up, o) for o in OFFSET_LIST[:count]]
    down = [every(has_down, o) for o in OFFSET_LIST[:count]]

    def device(offset, sign):
        return {name: p + sign * o for name, p, o in zip(AXES, place, offset)}

    basis_copy = pltpu.make_async_copy(bases_ref, basis, basis_sem)
    basis_copy.start()
    block_copies = [
        pltpu.make_async_copy(couplings_ref.at[s], blocks.at[s], block_sem.at[s]) for s in range(count)
    ]
    for s in LEFT_ORDER:
        block_copies[s].start()

    barrier = pltpu.get_barrier_semaphore()
    partners = jnp.int32(0)
    for s in range(count):
        for flag, sign in ((up[s], 1), (down[s], -1)):
            partners = partners + flag.astype(jnp.int32)

            @pl.when(flag)
            def _():
                pl.semaphore_signal(
                    barrier, inc=1, device_id=device(OFFSET_LIST[s], sign), device_id_type=pl.DeviceIdType.MESH
                )

    pl.semaphore_wait(barrier, partners)

    def rows(part):
        return pl.ds(part * half, half)

    def remote(src, dst, send, recv, offset, sign):
        return pltpu.make_async_remote_copy(
            src_ref=src, dst_ref=dst, send_sem=send, recv_sem=recv,
            device_id=device(offset, sign), device_id_type=pl.DeviceIdType.MESH,
        )

    def value_copy(slot, part, source, offset):
        return remote(
            source.at[rows(part)], values.at[slot, rows(part)],
            value_send.at[slot, part], value_recv.at[slot, part], offset, -1,
        )

    sent = {}
    for s in (X, Y, Z):
        for part in (0, 1):
            sent[s, part] = (value_copy(s, part, vectors_ref, OFFSET_LIST[s]), down[s])
    sent[XY, 0] = (value_copy(XY, 0, values.at[X], OFFSET_LIST[Y]), jnp.logical_and(has_up[0], has_down[1]))
    sent[XY, 1] = (value_copy(XY, 1, values.at[Y], OFFSET_LIST[X]), jnp.logical_and(has_up[1], has_down[0]))
    for part in (0, 1):
        sent[XZ, part] = (
            value_copy(XZ, part, values.at[X], OFFSET_LIST[Z]), jnp.logical_and(has_up[0], has_down[2]),
        )

    def start(slot, part):
        copy, flag = sent[slot, part]
        pl.when(flag)(copy.start)

    def arrived(slot, part):
        pl.when(up[slot])(sent[slot, part][0].wait_recv)

    left_copies = [
        remote(left_out.at[s], left_in.at[s], left_send.at[s], left_recv.at[s], OFFSET_LIST[s], 1)
        for s in range(count)
    ]
    back_copies = [
        remote(back_out.at[s], back_in.at[s], back_send.at[s], back_recv.at[s], OFFSET_LIST[s], -1)
        for s in range(count)
    ]

    start(X, 0)
    start(Y, 1)
    start(Z, 0)
    start(X, 1)
    start(Y, 0)
    start(Z, 1)

    total[...] = jnp.zeros_like(total)
    back_in[...] = jnp.zeros_like(back_in)
    basis_copy.wait()
    columns = lax.broadcasted_iota(jnp.int32, (m, k), 1)
    masked = jnp.where(columns < ranks_ref[0], basis[...], 0.0)
    high, low = split2(masked)
    basis_parts[:, :k] = high
    basis_parts[:, k:] = low
    high, low = split2(masked.T)
    stacked[:k] = high
    stacked[k:] = low

    wide = min(512, m)
    for s in LEFT_ORDER:
        block_copies[s].wait()

        @pl.when(up[s])
        def _():
            @pl.loop(0, m // wide)
            def _(step):
                there = pl.ds(pl.multiple_of(step * wide, wide), wide)
                both = dot32(stacked[...], blocks[s, :, there])
                left_out[s, :, there] = both[:k] + both[k:]

            left_copies[s].start()

    tall = min(512, m)

    def apply(slot, part):
        @pl.when(up[slot])
        def _():
            high, low = split2(values[slot, rows(part)])
            pair = jnp.concatenate([high, low], axis=1)

            @pl.loop(0, m // tall)
            def _(step):
                there = pl.ds(pl.multiple_of(step * tall, tall), tall)
                both = dot32(blocks[slot, there, rows(part)], pair)
                total[there] += both[:, :r] + both[:, r:]

    def project(slot):
        @pl.when(down[slot])
        def _():
            left_copies[slot].wait_recv()
            high, low = split2(left_in[slot])
            first = dot32(high, basis_parts[...])
            second = dot32(low, basis_parts[:, :k])
            back_out[slot] = first[:, :k] + first[:, k:] + second
            back_copies[slot].start()

    arrived(X, 0)
    start(XY, 0)
    start(XZ, 0)
    arrived(Y, 1)
    start(XY, 1)
    arrived(Z, 0)
    arrived(Z, 1)
    apply(Z, 0)
    apply(Z, 1)
    apply(X, 0)
    apply(Y, 1)
    project(Z)
    project(Y)
    project(XY)
    arrived(X, 1)
    start(XZ, 1)
    arrived(Y, 0)
    apply(X, 1)
    apply(Y, 0)
    arrived(XZ, 0)
    apply(XZ, 0)
    project(X)
    arrived(XZ, 1)
    apply(XZ, 1)
    arrived(XY, 0)
    apply(XY, 0)
    arrived(XY, 1)
    apply(XY, 1)
    applied_ref[...] = total[...]
    project(XZ)
    for s in range(count):
        pl.when(up[s])(back_copies[s].wait_recv)
    projected_ref[...] = back_in[...]
    for s in range(count):
        for part in (0, 1):
            copy, flag = sent[s, part]
            pl.when(flag)(copy.wait_send)
        pl.when(up[s])(left_copies[s].wait_send)
        pl.when(down[s])(back_copies[s].wait_send)


def solution(mesh):
    sizes = tuple(mesh.shape[name] for name in AXES)

    def local(bases, ranks, couplings, vectors):
        m, k = bases.shape[-2:]
        count = couplings.shape[3]
        r = vectors.shape[-1]
        f32, bf16 = jnp.float32, jnp.bfloat16
        dma = pltpu.SemaphoreType.DMA
        projected, applied = pl.pallas_call(
            functools.partial(kernel, sizes),
            out_shape=(
                jax.ShapeDtypeStruct((count, k, k), f32),
                jax.ShapeDtypeStruct((m, r), f32),
            ),
            in_specs=[pl.BlockSpec(memory_space=pltpu.SMEM)] + [pl.BlockSpec(memory_space=pl.ANY)] * 3,
            out_specs=(pl.BlockSpec(memory_space=pltpu.VMEM),) * 2,
            scratch_shapes=[
                pltpu.VMEM((m, k), f32),
                pltpu.VMEM((2 * k, m), bf16),
                pltpu.VMEM((m, 2 * k), bf16),
                pltpu.VMEM((count, m, m), bf16),
                pltpu.VMEM((count, m, r), f32),
                pltpu.VMEM((count, k, m), f32),
                pltpu.VMEM((count, k, m), f32),
                pltpu.VMEM((count, k, k), f32),
                pltpu.VMEM((count, k, k), f32),
                pltpu.VMEM((m, r), f32),
                dma,
                dma((count,)),
                dma((count, 2)),
                dma((count, 2)),
                dma((count,)),
                dma((count,)),
                dma((count,)),
                dma((count,)),
            ],
            compiler_params=pltpu.CompilerParams(collective_id=0, has_side_effects=True),
        )(
            ranks.reshape(1),
            bases.reshape(m, k),
            couplings.reshape(count, m, m),
            vectors.reshape(m, r),
        )
        return (
            projected.reshape(1, 1, 1, count, k, k),
            applied.reshape(1, 1, 1, m, r),
        )

    return jax.shard_map(
        local,
        mesh=mesh,
        in_specs=(
            P("gx", "gy", "gz", None, None),
            P("gx", "gy", "gz"),
            P("gx", "gy", "gz", None, None, None),
            P("gx", "gy", "gz", None, None),
        ),
        out_specs=(P("gx", "gy", "gz", None, None, None), P("gx", "gy", "gz", None, None)),
        check_vma=False,
    )
```

```python
import functools

import jax
import jax.numpy as jnp
from jax import lax
from jax.experimental import pallas as pl
from jax.experimental.pallas import tpu as pltpu
from jax.sharding import PartitionSpec as P

OFFSET_LIST = ((1, 0, 0), (0, 1, 0), (0, 0, 1), (1, 1, 0), (1, 0, 1), (0, 1, 1), (1, 1, 1))
AXES = ("gx", "gy", "gz")
X, Y, Z, XY, XZ = range(5)
LEFT_ORDER = (XY, Y, X, XZ, Z)


def split2(value):
    high = value.astype(jnp.bfloat16)
    low = (value - high.astype(jnp.float32)).astype(jnp.bfloat16)
    return high, low


def dot32(left, right):
    return jnp.dot(left, right, preferred_element_type=jnp.float32)


def kernel(
    sizes, ranks_ref, bases_ref, couplings_ref, vectors_ref, projected_ref, applied_ref,
    basis, stacked, basis_parts, blocks, values, left_out, left_in, relay, back_out, back_in,
    basis_sem, block_sem, value_send, value_recv, left_send, left_recv, relay_send, relay_recv, back_send, back_recv,
):
    count, m, k = blocks.shape[0], basis.shape[0], basis.shape[1]
    r = applied_ref.shape[1]
    half = m // 2
    place = [lax.axis_index(name) for name in AXES]
    has_up = [p < n - 1 for p, n in zip(place, sizes)]
    has_down = [p > 0 for p in place]

    def every(flags, offset):
        out = None
        for flag, o in zip(flags, offset):
            if o:
                out = flag if out is None else jnp.logical_and(out, flag)
        return out

    up = [every(has_up, o) for o in OFFSET_LIST[:count]]
    down = [every(has_down, o) for o in OFFSET_LIST[:count]]

    def device(offset, sign):
        return {name: p + sign * o for name, p, o in zip(AXES, place, offset)}

    basis_copy = pltpu.make_async_copy(bases_ref, basis, basis_sem)
    basis_copy.start()
    block_copies = [
        pltpu.make_async_copy(couplings_ref.at[s], blocks.at[s], block_sem.at[s]) for s in range(count)
    ]
    for s in LEFT_ORDER:
        block_copies[s].start()

    barrier = pltpu.get_barrier_semaphore()
    partners = jnp.int32(0)
    for s in range(count):
        for flag, sign in ((up[s], 1), (down[s], -1)):
            partners = partners + flag.astype(jnp.int32)

            @pl.when(flag)
            def _():
                pl.semaphore_signal(
                    barrier, inc=1, device_id=device(OFFSET_LIST[s], sign), device_id_type=pl.DeviceIdType.MESH
                )

    pl.semaphore_wait(barrier, partners)

    def rows(part):
        return pl.ds(part * half, half)

    def remote(src, dst, send, recv, offset, sign):
        return pltpu.make_async_remote_copy(
            src_ref=src, dst_ref=dst, send_sem=send, recv_sem=recv,
            device_id=device(offset, sign), device_id_type=pl.DeviceIdType.MESH,
        )

    def value_copy(slot, part, source, offset):
        return remote(
            source.at[rows(part)], values.at[slot, rows(part)],
            value_send.at[slot, part], value_recv.at[slot, part], offset, -1,
        )

    sent = {}
    for s in (X, Y, Z):
        for part in (0, 1):
            sent[s, part] = (value_copy(s, part, vectors_ref, OFFSET_LIST[s]), down[s])
    sent[XY, 0] = (value_copy(XY, 0, values.at[X], OFFSET_LIST[Y]), jnp.logical_and(has_up[0], has_down[1]))
    sent[XY, 1] = (value_copy(XY, 1, values.at[Y], OFFSET_LIST[X]), jnp.logical_and(has_up[1], has_down[0]))
    for part in (0, 1):
        sent[XZ, part] = (
            value_copy(XZ, part, values.at[X], OFFSET_LIST[Z]), jnp.logical_and(has_up[0], has_down[2]),
        )

    def start(slot, part):
        copy, flag = sent[slot, part]
        pl.when(flag)(copy.start)

    def arrived(slot, part):
        pl.when(up[slot])(sent[slot, part][0].wait_recv)

    relays = [
        remote(left_out.at[XY, part], relay.at[part], relay_send.at[part], relay_recv.at[part], OFFSET_LIST[s], 1)
        for part, s in ((0, X), (1, Y))
    ]
    onward = [
        remote(relay.at[part], left_in.at[XY, part], left_send.at[XY, part], left_recv.at[XY, part], OFFSET_LIST[s], 1)
        for part, s in ((0, Y), (1, X))
    ]
    passed = (
        ((relays[0], onward[0]), jnp.logical_and(has_down[0], has_up[1])),
        ((relays[1], onward[1]), jnp.logical_and(has_down[1], has_up[0])),
    )
    left_copies = [
        relays if s == XY else [
            remote(left_out.at[s], left_in.at[s], left_send.at[s, 0], left_recv.at[s, 0], OFFSET_LIST[s], 1)
        ]
        for s in range(count)
    ]
    back_copies = [
        remote(back_out.at[s], back_in.at[s], back_send.at[s], back_recv.at[s], OFFSET_LIST[s], -1)
        for s in range(count)
    ]

    start(X, 0)
    start(Y, 1)
    start(Z, 0)
    start(X, 1)
    start(Y, 0)
    start(Z, 1)

    basis_copy.wait()
    columns = lax.broadcasted_iota(jnp.int32, (m, k), 1)
    masked = jnp.where(columns < ranks_ref[0, 0, 0], basis[...], 0.0)
    high, low = split2(masked)
    basis_parts[:, :k] = high
    basis_parts[:, k:] = low
    high, low = split2(masked.T)
    stacked[:k] = high
    stacked[k:] = low

    for s in LEFT_ORDER:
        block_copies[s].wait()

        @pl.when(up[s])
        def _():
            @pl.loop(0, 2)
            def _(part):
                there = pl.ds(pl.multiple_of(part * half, half), half)
                both = dot32(stacked[...], blocks[s, :, there])
                left_out[s, part] = both[:k] + both[k:]

            for copy in left_copies[s]:
                copy.start()

    applied_ref[...] = jnp.zeros_like(applied_ref)
    for s in range(count):

        @pl.when(jnp.logical_not(up[s]))
        def _():
            back_in[s] = jnp.zeros((k, k), jnp.float32)

    for copy, flag in passed:
        @pl.when(flag)
        def _():
            copy[0].wait_recv()
            copy[1].start()

    tall = min(512, m)

    def apply(slot, part):
        @pl.when(up[slot])
        def _():
            high, low = split2(values[slot, rows(part)])
            pair = jnp.concatenate([high, low], axis=1)

            @pl.loop(0, m // tall)
            def _(step):
                there = pl.ds(pl.multiple_of(step * tall, tall), tall)
                both = dot32(blocks[slot, there, rows(part)], pair)
                applied_ref[there] += both[:, :r] + both[:, r:]

    def project(slot):
        @pl.when(down[slot])
        def _():
            for copy in onward if slot == XY else left_copies[slot]:
                copy.wait_recv()
            out = None
            for part in (0, 1):
                high, low = split2(left_in[slot, part])
                first = dot32(high, basis_parts[rows(part)])
                term = first[:, :k] + first[:, k:] + dot32(low, basis_parts[rows(part), :k])
                out = term if out is None else out + term
            back_out[slot] = out
            back_copies[slot].start()

    arrived(X, 0)
    start(XY, 0)
    start(XZ, 0)
    arrived(Y, 1)
    start(XY, 1)
    arrived(Z, 0)
    arrived(Z, 1)
    apply(Z, 0)
    apply(Z, 1)
    apply(X, 0)
    apply(Y, 1)
    project(Z)
    project(Y)
    project(XY)
    arrived(X, 1)
    start(XZ, 1)
    arrived(Y, 0)
    apply(X, 1)
    apply(Y, 0)
    arrived(XZ, 0)
    apply(XZ, 0)
    project(X)
    arrived(XZ, 1)
    apply(XZ, 1)
    project(XZ)
    arrived(XY, 0)
    apply(XY, 0)
    arrived(XY, 1)
    apply(XY, 1)
    for s in range(count):
        pl.when(up[s])(back_copies[s].wait_recv)
    projected_ref[...] = back_in[...]
    for s in range(count):
        for part in (0, 1):
            copy, flag = sent[s, part]
            pl.when(flag)(copy.wait_send)
        for copy in left_copies[s]:
            pl.when(up[s])(copy.wait_send)
        pl.when(down[s])(back_copies[s].wait_send)
    for copy, flag in passed:
        pl.when(flag)(copy[1].wait_send)


def solution(mesh):
    sizes = tuple(mesh.shape[name] for name in AXES)

    def local(bases, ranks, couplings, vectors):
        m, k = bases.shape[-2:]
        count = couplings.shape[3]
        r = vectors.shape[-1]
        f32, bf16 = jnp.float32, jnp.bfloat16
        dma = pltpu.SemaphoreType.DMA
        projected, applied = pl.pallas_call(
            functools.partial(kernel, sizes),
            out_shape=(
                pltpu.VMEM((count, k, k), f32),
                pltpu.VMEM((m, r), f32),
            ),
            in_specs=[pl.BlockSpec(memory_space=pltpu.SMEM)] + [pl.BlockSpec(memory_space=pltpu.HBM)] * 3,
            out_specs=(pl.BlockSpec(memory_space=pltpu.VMEM),) * 2,
            scratch_shapes=[
                pltpu.VMEM((m, k), f32),
                pltpu.VMEM((2 * k, m), bf16),
                pltpu.VMEM((m, 2 * k), bf16),
                pltpu.VMEM((count, m, m), bf16),
                pltpu.VMEM((count, m, r), f32),
                pltpu.VMEM((count, 2, k, m // 2), f32),
                pltpu.VMEM((count, 2, k, m // 2), f32),
                pltpu.VMEM((2, k, m // 2), f32),
                pltpu.VMEM((count, k, k), f32),
                pltpu.VMEM((count, k, k), f32),
                dma,
                dma((count,)),
                dma((count, 2)),
                dma((count, 2)),
                dma((count, 2)),
                dma((count, 2)),
                dma((2,)),
                dma((2,)),
                dma((count,)),
                dma((count,)),
            ],
            compiler_params=pltpu.CompilerParams(collective_id=0, has_side_effects=True, vmem_limit_bytes=64000 << 10),
        )(
            ranks,
            bases.reshape(m, k),
            couplings.reshape(count, m, m),
            vectors.reshape(m, r),
        )
        return (
            projected.reshape(1, 1, 1, count, k, k),
            applied.reshape(1, 1, 1, m, r),
        )

    return jax.shard_map(
        local,
        mesh=mesh,
        in_specs=(
            P("gx", "gy", "gz", None, None),
            P("gx", "gy", "gz"),
            P("gx", "gy", "gz", None, None, None),
            P("gx", "gy", "gz", None, None),
        ),
        out_specs=(P("gx", "gy", "gz", None, None, None), P("gx", "gy", "gz", None, None)),
        check_vma=False,
    )
```
